64 devices in a mesh: dp: 4 (over x, y), sp: 16 (over z, core).
Axes of the slice: x: 2, y: 2, z: 8, core: 2. Of those that a mesh axis runs over, the one named last changes fastest.
The devices are a block of a 4x4x8 slice.
Arguments:
- q: bfloat16 [128, 16, 256], P('dp'), parts along dimension 0
- k: bfloat16 [128, 4096, 8, 256], P('dp', 'sp'), parts along dimension 0
- v: bfloat16 [128, 4096, 8, 256], P('dp', 'sp'), parts along dimension 0
Outputs:
- q: bfloat16 [128, 16, 256], P('dp'), parts along dimension 0
There are 4 independent parts. The reference program is written for one: setup_inputs(seed, part) draws one part's arguments, and reference() takes and returns one part's arrays. A program takes and returns all parts, laid end to end along the dimension named above; each array names one.
All inputs are finite; a program needn't handle non-finite values.
Results may differ from the reference program's by a relative error of at most 0.012.
Values are sent between devices in bfloat16 or wider.
A program may use at most 768 MiB of HBM per device.

```python
import jax
import jax.numpy as jnp

BATCH = 32
CACHE = 4096
HEADS = 16
KV_HEADS = 8
HEAD = 256


def setup_inputs(seed: int = 0, part: int = 0) -> dict:
    kq, kk, kv = (jax.random.fold_in(k, part) for k in jax.random.split(jax.random.key(seed), 3))
    return {
        "q": (3 * jax.random.normal(kq, (BATCH, HEADS, HEAD), jnp.float32)).astype(jnp.bfloat16),
        "k": jax.random.normal(kk, (BATCH, CACHE, KV_HEADS, HEAD), jnp.float32).astype(jnp.bfloat16),
        "v": jax.random.normal(kv, (BATCH, CACHE, KV_HEADS, HEAD), jnp.float32).astype(jnp.bfloat16),
    }


def einsum(form, a, b):
    return jnp.einsum(form, a.astype(jnp.float32), b.astype(jnp.float32))


def reference(q, k, v):
    grouped = q.reshape(BATCH, KV_HEADS, -1, HEAD)
    scores = einsum("bgsd,bugd->bgsu", grouped, k) * HEAD**-0.5
    weights = jax.nn.softmax(scores, -1).astype(jnp.bfloat16)
    return einsum("bgsu,bugd->bgsd", weights, v).astype(jnp.bfloat16).reshape(BATCH, HEADS, HEAD)
```

```python
import functools

import jax
import jax.numpy as jnp
from jax import lax
from jax.experimental import pallas as pl
from jax.experimental.pallas import tpu as pltpu
from jax.sharding import PartitionSpec as P

MESH = pl.DeviceIdType.MESH
SLOTS = 6
LAG = 10
STRIDE = 5
BACK = 13


def kernel(n, p, rows, heads, head, kv, q_ref, k_hbm, v_hbm, out_ref, kbuf, vbuf, scores, weights, mine, stat, parts, stats,
           ksem, vsem, part_send, part_recv, stat_send, stat_recv, out_send, out_recv):
    me = lax.axis_index("sp")
    group = heads // kv
    scale = head ** -0.5

    def other(d):
        return lax.rem(me + d, p)

    def fetch_k(s, slot):
        return pltpu.make_async_copy(k_hbm.at[s], kbuf.at[slot], ksem.at[slot])

    def fetch_v(s, slot):
        return pltpu.make_async_copy(v_hbm.at[s], vbuf.at[slot], vsem.at[slot])

    for s in range(SLOTS):
        fetch_k(s, s).start()
        fetch_v(s, s).start()

    barrier = pltpu.get_barrier_semaphore()
    for d in range(1, p):
        pl.semaphore_signal(barrier, inc=1, device_id={"sp": other(d)}, device_id_type=MESH)

    row = lax.broadcasted_iota(jnp.int32, (heads, rows), 0)
    col = lax.broadcasted_iota(jnp.int32, (heads, rows), 1)
    own = (col % kv) == (row // group)
    half = heads // 2
    row1 = lax.broadcasted_iota(jnp.int32, (heads, 128), 0)
    col1 = lax.broadcasted_iota(jnp.int32, (heads, 128), 1)
    at_high, at_total = col1 == row1, col1 == row1 + 64

    def owner(s):
        return lax.rem(s * STRIDE, p)

    def score(s, slot):
        scores[...] = lax.dot_general(q_ref[s], kbuf[slot], (((1,), (1,)), ((), ())), preferred_element_type=jnp.float32)

    def soften(s):
        x = jnp.where(own, scores[...], -jnp.inf)
        high = jnp.max(x, axis=1, keepdims=True)
        w = jnp.exp((x - high) * scale)
        weights[...] = w.astype(jnp.bfloat16)
        total = jnp.sum(w, axis=1, keepdims=True)
        spread = jnp.where(at_high, high * scale, jnp.where(at_total, total, 0.0))
        stat[s] = spread[:half] + spread[half:]

    def mix(s, slot):
        mine[s] = jnp.dot(weights[...], vbuf[slot], preferred_element_type=jnp.float32).astype(jnp.bfloat16)

    def to_owner(s, src, dst, send, recv):
        who = owner(s)
        turn = s // p
        place = lax.rem(me - who - 1 + 2 * p, p)

        @pl.when(who != me)
        def _():
            pltpu.make_async_remote_copy(
                src_ref=src.at[s], dst_ref=dst.at[turn, place], send_sem=send, recv_sem=recv.at[turn], device_id={"sp": who}, device_id_type=MESH
            ).start()

    def send_stat(s):
        to_owner(s, stat, stats, stat_send, stat_recv)

    def send_part(s):
        to_owner(s, mine, parts, part_send, part_recv)

    def all_of(ref, sem):
        return pltpu.make_async_copy(ref, ref, sem)

    def together(s):
        turn = s // p
        all_of(stats.at[turn], stat_recv.at[turn]).wait()
        high, total = [], []
        for j in range(p):
            x = stat[s] if j == p - 1 else stats[turn, j]
            x = jnp.concatenate([x, x], axis=0)
            high.append(jnp.sum(jnp.where(at_high, x, 0.0), axis=1, keepdims=True))
            total.append(jnp.sum(jnp.where(at_total, x, 0.0), axis=1, keepdims=True))
        top = functools.reduce(jnp.maximum, high)
        share = [jnp.exp(h - top) for h in high]
        whole = functools.reduce(jnp.add, [a * t for a, t in zip(share, total)])
        all_of(parts.at[turn], part_recv.at[turn]).wait()
        seen = jnp.zeros((heads, head), jnp.float32)
        for j in range(p):
            x = mine[s] if j == p - 1 else parts[turn, j]
            seen = seen + x.astype(jnp.float32) * share[j]
        out_ref[s] = (seen / whole).astype(out_ref.dtype)
        for d in range(1, p):
            pltpu.make_async_remote_copy(
                src_ref=out_ref.at[s], dst_ref=out_ref.at[s], send_sem=out_send, recv_sem=out_recv, device_id={"sp": other(d)}, device_id_type=MESH
            ).start()

    fetch_k(0, 0).wait()
    score(0, 0)
    fetch_k(1, 1).wait()
    soften(0)
    score(1, 1)
    for s in (0, 1):
        fetch_k(s + SLOTS, s).start()
    pl.semaphore_wait(barrier, p - 1)
    send_stat(0)

    def body(s, _):
        kslot, vslot = lax.rem(s, SLOTS), lax.rem(s - 2, SLOTS)
        fetch_v(s - 2, vslot).wait()
        fetch_k(s, kslot).wait()
        mix(s - 2, vslot)
        soften(s - 1)
        score(s, kslot)

        @pl.when(s + SLOTS < n)
        def _():
            fetch_k(s + SLOTS, kslot).start()

        @pl.when(s - 2 + SLOTS < n)
        def _():
            fetch_v(s - 2 + SLOTS, vslot).start()

        send_stat(s - 1)
        send_part(s - 2)

        @pl.when((s >= LAG) & (owner(jnp.maximum(s - LAG, 0)) == me))
        def _():
            together(s - LAG)

        return 0

    lax.fori_loop(2, n, body, 0)
    slot = (n - 2) % SLOTS
    fetch_v(n - 2, slot).wait()
    mix(n - 2, slot)
    soften(n - 1)
    send_stat(n - 1)
    send_part(n - 2)
    slot = (n - 1) % SLOTS
    fetch_v(n - 1, slot).wait()
    mix(n - 1, slot)
    send_part(n - 1)
    last = n - p + lax.rem(me * BACK, p)

    @pl.when(last >= n - LAG)
    def _():
        together(last)

    turns = n // p
    all_of(out_ref.at[pl.ds(0, n - turns)], out_recv).wait()
    all_of(mine.at[pl.ds(0, n - turns)], part_send).wait()
    all_of(stat.at[pl.ds(0, n - turns)], stat_send).wait()
    all_of(out_ref.at[pl.ds(0, turns * (p - 1))], out_send).wait()


def solution(mesh):
    p = mesh.shape["sp"]

    def step(q, k, v):
        n, heads, head = q.shape
        tokens, kv = k.shape[1:3]
        rows = tokens * kv
        turns = n // p
        assert turns * p == n and (STRIDE * BACK) % p == 1
        return pl.pallas_call(
            functools.partial(kernel, n, p, rows, heads, head, kv),
            out_shape=jax.ShapeDtypeStruct(q.shape, q.dtype),
            in_specs=[pl.BlockSpec(memory_space=pltpu.VMEM), pl.BlockSpec(memory_space=pl.ANY), pl.BlockSpec(memory_space=pl.ANY)],
            out_specs=pl.BlockSpec(memory_space=pltpu.VMEM),
            scratch_shapes=[
                pltpu.VMEM((SLOTS, rows, head), jnp.bfloat16),
                pltpu.VMEM((SLOTS, rows, head), jnp.bfloat16),
                pltpu.VMEM((heads, rows), jnp.float32),
                pltpu.VMEM((heads, rows), jnp.bfloat16),
                pltpu.VMEM((n, heads, head), jnp.bfloat16),
                pltpu.VMEM((n, heads // 2, 128), jnp.float32),
                pltpu.VMEM((turns, p - 1, heads, head), jnp.bfloat16),
                pltpu.VMEM((turns, p - 1, heads // 2, 128), jnp.float32),
                pltpu.SemaphoreType.DMA((SLOTS,)),
                pltpu.SemaphoreType.DMA((SLOTS,)),
                pltpu.SemaphoreType.DMA,
                pltpu.SemaphoreType.DMA((turns,)),
                pltpu.SemaphoreType.DMA,
                pltpu.SemaphoreType.DMA((turns,)),
                pltpu.SemaphoreType.DMA,
                pltpu.SemaphoreType.DMA,
            ],
            compiler_params=pltpu.CompilerParams(vmem_limit_bytes=48 * 2**20, collective_id=0, has_side_effects=True),
            name="attend",
        )(q, k.reshape(n, rows, head), v.reshape(n, rows, head))

    return jax.shard_map(
        step,
        mesh=mesh,
        in_specs=(P("dp", None, None), P("dp", "sp", None, None), P("dp", "sp", None, None)),
        out_specs=P("dp", None, None),
        check_vma=False,
    )
```

```python
import functools

import jax
import jax.numpy as jnp
from jax import lax
from jax.experimental import pallas as pl
from jax.experimental.pallas import tpu as pltpu
from jax.sharding import PartitionSpec as P

MESH = pl.DeviceIdType.MESH
SLOTS = 6
OPEN = 8
FIRST = 24
LAG = 16
ORDER = (4, 10, 6, 12, 8, 14, 2, 11, 5, 9, 3, 13, 7, 0, 15, 1)


def kernel(n, p, rows, heads, head, kv, q_hbm, k_hbm, v_hbm, out_ref, q_ref, kbuf, vbuf, scores, weights, mine, stat, parts, stats,
           qsem, ksem, vsem, part_send, part_recv, stat_send, stat_recv, out_send, out_recv):
    me = lax.axis_index("sp")
    group = heads // kv
    scale = head ** -0.5

    def other(d):
        return lax.rem(me + d, p)

    def fetch_k(s, slot):
        return pltpu.make_async_copy(k_hbm.at[s], kbuf.at[slot], ksem.at[slot])

    def fetch_v(s, slot):
        return pltpu.make_async_copy(v_hbm.at[s], vbuf.at[slot], vsem.at[slot])

    fetch_q = pltpu.make_async_copy(q_hbm, q_ref, qsem)
    fetch_q.start()
    for s in range(SLOTS):
        fetch_k(s, s).start(priority=1)
        fetch_v(s, s).start(priority=1)

    barrier = pltpu.get_barrier_semaphore()
    for d in range(1, p):
        pl.semaphore_signal(barrier, inc=1, device_id={"sp": other(d)}, device_id_type=MESH)

    row = lax.broadcasted_iota(jnp.int32, (heads, rows), 0)
    col = lax.broadcasted_iota(jnp.int32, (heads, rows), 1)
    own = (col % kv) == (row // group)
    row1 = lax.broadcasted_iota(jnp.int32, (heads, 128), 0)
    col1 = lax.broadcasted_iota(jnp.int32, (heads, 128), 1)
    at_high, at_total = col1 == row1, col1 == row1 + 64

    def owner(s):
        j = lax.rem(s, p)
        return functools.reduce(jnp.add, [jnp.where(j == i, d, 0) for i, d in enumerate(ORDER)])

    def owned(turn):
        return turn * p + functools.reduce(jnp.add, [jnp.where(me == d, i, 0) for i, d in enumerate(ORDER)])

    def score(s, slot):
        scores[...] = lax.dot_general(q_ref[s], kbuf[slot], (((1,), (1,)), ((), ())), preferred_element_type=jnp.float32)

    def soften(s):
        x = jnp.where(own, scores[...], -jnp.inf)
        high = jnp.max(x, axis=1, keepdims=True)
        w = jnp.exp((x - high) * scale)
        weights[...] = w.astype(jnp.bfloat16)
        total = jnp.sum(w, axis=1, keepdims=True)
        spread = jnp.where(at_high, high * scale, jnp.where(at_total, total, 0.0))
        stat[s] = jnp.sum(spread, axis=0, keepdims=True)

    def mix(s, slot):
        mine[s] = jnp.dot(weights[...], vbuf[slot], preferred_element_type=jnp.float32).astype(jnp.bfloat16)

    def to_owner(s, src, dst, send, recv):
        who = owner(s)
        turn = s // p
        place = lax.rem(me - who - 1 + 2 * p, p)

        @pl.when(who != me)
        def _():
            pltpu.make_async_remote_copy(
                src_ref=src.at[s], dst_ref=dst.at[turn, place], send_sem=send, recv_sem=recv.at[turn], device_id={"sp": who}, device_id_type=MESH
            ).start()

    def send_stat(s):
        to_owner(s, stat, stats, stat_send, stat_recv)

    def send_part(s):
        to_owner(s, mine, parts, part_send, part_recv)

    def all_of(ref, sem):
        return pltpu.make_async_copy(ref, ref, sem)

    def together(s):
        turn = s // p
        all_of(stats.at[turn], stat_recv.at[turn]).wait()
        high, total = [], []
        for j in range(p):
            x = stat[s] if j == p - 1 else stats[turn, j]
            high.append(jnp.sum(jnp.where(at_high, x, 0.0), axis=1, keepdims=True))
            total.append(jnp.sum(jnp.where(at_total, x, 0.0), axis=1, keepdims=True))
        top = functools.reduce(jnp.maximum, high)
        share = [jnp.exp(h - top) for h in high]
        whole = functools.reduce(jnp.add, [a * t for a, t in zip(share, total)])
        all_of(parts.at[turn], part_recv.at[turn]).wait()
        seen = jnp.zeros((heads, head), jnp.float32)
        for j in range(p):
            x = mine[s] if j == p - 1 else parts[turn, j]
            seen = seen + x.astype(jnp.float32) * share[j]
        out_ref[s] = (seen / whole).astype(out_ref.dtype)
        for d in range(1, p):
            pltpu.make_async_remote_copy(
                src_ref=out_ref.at[s], dst_ref=out_ref.at[s], send_sem=out_send, recv_sem=out_recv, device_id={"sp": other(d)}, device_id_type=MESH
            ).start()

    fetch_q.wait()
    fetch_k(0, 0).wait()
    score(0, 0)
    fetch_k(1, 1).wait()
    soften(0)
    score(1, 1)
    for s in (0, 1):
        fetch_k(s + SLOTS, s).start(priority=1)

    def body(s, _):
        kslot, vslot = lax.rem(s, SLOTS), lax.rem(s - 2, SLOTS)
        fetch_v(s - 2, vslot).wait()
        fetch_k(s, kslot).wait()
        mix(s - 2, vslot)
        soften(s - 1)
        score(s, kslot)

        @pl.when(s + SLOTS < n)
        def _():
            fetch_k(s + SLOTS, kslot).start(priority=1)

        @pl.when(s - 2 + SLOTS < n)
        def _():
            fetch_v(s - 2 + SLOTS, vslot).start(priority=1)

        @pl.when(s == OPEN)
        def _():
            pl.semaphore_wait(barrier, p - 1)

            def late(u, _):
                send_stat(u)
                send_part(u)
                return 0

            lax.fori_loop(0, OPEN - 2, late, 0)
            send_stat(OPEN - 2)

        @pl.when(s >= OPEN)
        def _():
            send_stat(s - 1)
            send_part(s - 2)

        @pl.when(s == FIRST)
        def _():
            together(owned(0))

        @pl.when((s >= p + LAG) & (owner(jnp.maximum(s - LAG, 0)) == me))
        def _():
            together(s - LAG)

        return 0

    lax.fori_loop(2, n, body, 0)
    slot = (n - 2) % SLOTS
    fetch_v(n - 2, slot).wait()
    mix(n - 2, slot)
    soften(n - 1)
    send_stat(n - 1)
    send_part(n - 2)
    slot = (n - 1) % SLOTS
    fetch_v(n - 1, slot).wait()
    mix(n - 1, slot)
    send_part(n - 1)
    @pl.when(owned(1) >= n - LAG)
    def _():
        together(owned(1))

    turns = n // p
    all_of(out_ref.at[pl.ds(0, n - turns)], out_recv).wait()
    all_of(mine.at[pl.ds(0, n - turns)], part_send).wait()
    all_of(stat.at[pl.ds(0, n - turns)], stat_send).wait()
    all_of(out_ref.at[pl.ds(0, turns * (p - 1))], out_send).wait()


def solution(mesh):
    p = mesh.shape["sp"]

    def step(q, k, v):
        n, heads, head = q.shape
        tokens, kv = k.shape[1:3]
        rows = tokens * kv
        turns = n // p
        assert n == 2 * p and sorted(ORDER) == list(range(p)) and FIRST >= p + 2
        return pl.pallas_call(
            functools.partial(kernel, n, p, rows, heads, head, kv),
            out_shape=jax.ShapeDtypeStruct(q.shape, q.dtype),
            in_specs=[pl.BlockSpec(memory_space=pltpu.HBM)] * 3,
            out_specs=pl.BlockSpec(memory_space=pltpu.VMEM),
            scratch_shapes=[
                pltpu.VMEM((n, heads, head), jnp.bfloat16),
                pltpu.VMEM((SLOTS, rows, head), jnp.bfloat16),
                pltpu.VMEM((SLOTS, rows, head), jnp.bfloat16),
                pltpu.VMEM((heads, rows), jnp.float32),
                pltpu.VMEM((heads, rows), jnp.bfloat16),
                pltpu.VMEM((n, heads, head), jnp.bfloat16),
                pltpu.VMEM((n, 1, 128), jnp.float32),
                pltpu.VMEM((turns, p - 1, heads, head), jnp.bfloat16),
                pltpu.VMEM((turns, p - 1, 1, 128), jnp.float32),
                pltpu.SemaphoreType.DMA,
                pltpu.SemaphoreType.DMA((SLOTS,)),
                pltpu.SemaphoreType.DMA((SLOTS,)),
                pltpu.SemaphoreType.DMA,
                pltpu.SemaphoreType.DMA((turns,)),
                pltpu.SemaphoreType.DMA,
                pltpu.SemaphoreType.DMA((turns,)),
                pltpu.SemaphoreType.DMA,
                pltpu.SemaphoreType.DMA,
            ],
            compiler_params=pltpu.CompilerParams(vmem_limit_bytes=48 * 2**20, collective_id=0, has_side_effects=True),
            name="attend",
        )(pltpu.with_memory_space_constraint(q, pltpu.HBM), k.reshape(n, rows, head), v.reshape(n, rows, head))

    return jax.shard_map(
        step,
        mesh=mesh,
        in_specs=(P("dp", None, None), P("dp", "sp", None, None), P("dp", "sp", None, None)),
        out_specs=P("dp", None, None),
        check_vma=False,
    )
```

```python
import functools

import jax
import jax.numpy as jnp
from jax import lax
from jax.experimental import pallas as pl
from jax.experimental.pallas import tpu as pltpu
from jax.sharding import PartitionSpec as P

MESH = pl.DeviceIdType.MESH
SLOTS = 6
OPEN = 8
FIRST = 24
LAG = 16
ORDER = (4, 10, 6, 12, 8, 14, 2, 11, 7, 9, 3, 13, 5, 0, 15, 1)


def kernel(n, p, rows, heads, head, kv, q_hbm, k_hbm, v_hbm, out_ref, q_ref, kbuf, vbuf, scores, weights, mine, stat, parts, stats,
           qsem, ksem, vsem, part_send, part_recv, stat_send, stat_recv, out_send, out_recv):
    me = lax.axis_index("sp")
    group = heads // kv
    scale = head ** -0.5

    def other(d):
        return lax.rem(me + d, p)

    def fetch_k(s, slot):
        return pltpu.make_async_copy(k_hbm.at[s], kbuf.at[slot], ksem.at[slot])

    def fetch_v(s, slot):
        return pltpu.make_async_copy(v_hbm.at[s], vbuf.at[slot], vsem.at[slot])

    fetch_q = pltpu.make_async_copy(q_hbm, q_ref, qsem)
    fetch_q.start()
    for s in range(SLOTS):
        fetch_k(s, s).start(priority=1)
        fetch_v(s, s).start(priority=1)

    barrier = pltpu.get_barrier_semaphore()
    for d in range(1, p):
        pl.semaphore_signal(barrier, inc=1, device_id={"sp": other(d)}, device_id_type=MESH)

    row = lax.broadcasted_iota(jnp.int32, (heads, rows), 0)
    col = lax.broadcasted_iota(jnp.int32, (heads, rows), 1)
    own = (col % kv) == (row // group)
    row1 = lax.broadcasted_iota(jnp.int32, (heads, 128), 0)
    col1 = lax.broadcasted_iota(jnp.int32, (heads, 128), 1)
    at_high, at_total = col1 == row1, col1 == row1 + 64

    def owner(s):
        j = lax.rem(s, p)
        return functools.reduce(jnp.add, [jnp.where(j == i, d, 0) for i, d in enumerate(ORDER)])

    def owned(turn):
        return turn * p + functools.reduce(jnp.add, [jnp.where(me == d, i, 0) for i, d in enumerate(ORDER)])

    def score(s, slot):
        scores[...] = lax.dot_general(q_ref[s], kbuf[slot], (((1,), (1,)), ((), ())), preferred_element_type=jnp.float32)

    def soften(s):
        x = jnp.where(own, scores[...], -jnp.inf)
        high = jnp.max(x, axis=1, keepdims=True)
        w = jnp.exp((x - high) * scale)
        weights[...] = w.astype(jnp.bfloat16)
        total = jnp.sum(w, axis=1, keepdims=True)
        spread = jnp.where(at_high, high * scale, jnp.where(at_total, total, 0.0))
        stat[s] = jnp.sum(spread, axis=0, keepdims=True)

    def mix(s, slot, pieces=1):
        step = rows // pieces
        got = [jnp.dot(weights[:, i:i + step], vbuf[slot, i:i + step], preferred_element_type=jnp.float32) for i in range(0, rows, step)]
        mine[s] = functools.reduce(jnp.add, got).astype(jnp.bfloat16)

    def to_owner(s, who, src, dst, send, recv):
        turn = s // p
        place = lax.rem(me - who - 1 + 2 * p, p)

        @pl.when(who != me)
        def _():
            pltpu.make_async_remote_copy(
                src_ref=src.at[s], dst_ref=dst.at[turn, place], send_sem=send, recv_sem=recv.at[turn], device_id={"sp": who}, device_id_type=MESH
            ).start()

    def send_stat(s, who):
        to_owner(s, who, stat, stats, stat_send, stat_recv)

    def send_part(s, who):
        to_owner(s, who, mine, parts, part_send, part_recv)

    def all_of(ref, sem):
        return pltpu.make_async_copy(ref, ref, sem)

    def together(s):
        turn = s // p
        all_of(stats.at[turn], stat_recv.at[turn]).wait()
        rows = [stat[s] if j == p - 1 else stats[turn, j] for j in range(p)]
        top = functools.reduce(jnp.maximum, rows)
        share = [jnp.exp(x - top) for x in rows]
        whole = functools.reduce(jnp.add, [a * pltpu.roll(x, 64, 1) for a, x in zip(share, rows)])
        share = [jnp.sum(jnp.where(at_high, a / whole, 0.0), axis=1, keepdims=True) for a in share]
        all_of(parts.at[turn], part_recv.at[turn]).wait()
        seen = jnp.zeros((heads, head), jnp.float32)
        for j in range(p):
            x = mine[s] if j == p - 1 else parts[turn, j]
            seen = seen + x.astype(jnp.float32) * share[j]
        out_ref[s] = seen.astype(out_ref.dtype)
        for d in sorted(range(1, p), key=lambda d: min(d, p - d)):
            pltpu.make_async_remote_copy(
                src_ref=out_ref.at[s], dst_ref=out_ref.at[s], send_sem=out_send, recv_sem=out_recv, device_id={"sp": other(d)}, device_id_type=MESH
            ).start()

    fetch_q.wait()
    fetch_k(0, 0).wait()
    score(0, 0)
    fetch_k(1, 1).wait()
    soften(0)
    score(1, 1)
    for s in (0, 1):
        fetch_k(s + SLOTS, s).start(priority=1)

    def body(s, before):
        who = owner(s - 1)
        kslot, vslot = lax.rem(s, SLOTS), lax.rem(s - 2, SLOTS)
        fetch_v(s - 2, vslot).wait()
        fetch_k(s, kslot).wait()
        mix(s - 2, vslot)
        soften(s - 1)
        score(s, kslot)

        @pl.when(s + SLOTS < n)
        def _():
            fetch_k(s + SLOTS, kslot).start(priority=1)

        @pl.when(s - 2 + SLOTS < n)
        def _():
            fetch_v(s - 2 + SLOTS, vslot).start(priority=1)

        @pl.when(s == OPEN)
        def _():
            pl.semaphore_wait(barrier, p - 1)

            def late(u, _):
                who = owner(u)
                send_stat(u, who)
                send_part(u, who)
                return 0

            lax.fori_loop(0, OPEN - 2, late, 0)
            send_stat(OPEN - 2, ORDER[(OPEN - 2) % p])

        @pl.when(s >= OPEN)
        def _():
            send_stat(s - 1, who)
            send_part(s - 2, before)

        @pl.when(s == FIRST)
        def _():
            together(owned(0))

        @pl.when((s >= p + LAG) & (owner(jnp.maximum(s - LAG, 0)) == me))
        def _():
            together(s - LAG)

        return who

    lax.fori_loop(2, n, body, jnp.int32(ORDER[0]))
    slot = (n - 2) % SLOTS
    fetch_v(n - 2, slot).wait()
    mix(n - 2, slot, 2)
    soften(n - 1)
    send_stat(n - 1, ORDER[p - 1])
    send_part(n - 2, ORDER[p - 2])
    slot = (n - 1) % SLOTS
    fetch_v(n - 1, slot).wait()
    mix(n - 1, slot, 2)
    send_part(n - 1, ORDER[p - 1])
    @pl.when(owned(1) >= n - LAG)
    def _():
        together(owned(1))

    turns = n // p
    all_of(out_ref.at[pl.ds(0, n - turns)], out_recv).wait()
    all_of(mine.at[pl.ds(0, n - turns)], part_send).wait()
    all_of(stat.at[pl.ds(0, n - turns)], stat_send).wait()
    all_of(out_ref.at[pl.ds(0, turns * (p - 1))], out_send).wait()


def solution(mesh):
    p = mesh.shape["sp"]

    def step(q, k, v):
        n, heads, head = q.shape
        tokens, kv = k.shape[1:3]
        rows = tokens * kv
        turns = n // p
        assert n == 2 * p and sorted(ORDER) == list(range(p)) and FIRST >= p + 2
        return pl.pallas_call(
            functools.partial(kernel, n, p, rows, heads, head, kv),
            out_shape=jax.ShapeDtypeStruct(q.shape, q.dtype),
            in_specs=[pl.BlockSpec(memory_space=pltpu.HBM)] * 3,
            out_specs=pl.BlockSpec(memory_space=pltpu.VMEM),
            scratch_shapes=[
                pltpu.VMEM((n, heads, head), jnp.bfloat16),
                pltpu.VMEM((SLOTS, rows, head), jnp.bfloat16),
                pltpu.VMEM((SLOTS, rows, head), jnp.bfloat16),
                pltpu.VMEM((heads, rows), jnp.float32),
                pltpu.VMEM((heads, rows), jnp.bfloat16),
                pltpu.VMEM((n, heads, head), jnp.bfloat16),
                pltpu.VMEM((n, 1, 128), jnp.float32),
                pltpu.VMEM((turns, p - 1, heads, head), jnp.bfloat16),
                pltpu.VMEM((turns, p - 1, 1, 128), jnp.float32),
                pltpu.SemaphoreType.DMA,
                pltpu.SemaphoreType.DMA((SLOTS,)),
                pltpu.SemaphoreType.DMA((SLOTS,)),
                pltpu.SemaphoreType.DMA,
                pltpu.SemaphoreType.DMA((turns,)),
                pltpu.SemaphoreType.DMA,
                pltpu.SemaphoreType.DMA((turns,)),
                pltpu.SemaphoreType.DMA,
                pltpu.SemaphoreType.DMA,
            ],
            compiler_params=pltpu.CompilerParams(vmem_limit_bytes=48 * 2**20, collective_id=0, has_side_effects=True),
            name="attend",
        )(pltpu.with_memory_space_constraint(q, pltpu.HBM), k.reshape(n, rows, head), v.reshape(n, rows, head))

    return jax.shard_map(
        step,
        mesh=mesh,
        in_specs=(P("dp", None, None), P("dp", "sp", None, None), P("dp", "sp", None, None)),
        out_specs=P("dp", None, None),
        check_vma=False,
    )
```

```python
import functools

import jax
import jax.numpy as jnp
from jax import lax
from jax.experimental import pallas as pl
from jax.experimental.pallas import tpu as pltpu
from jax.sharding import PartitionSpec as P

MESH = pl.DeviceIdType.MESH
SLOTS = 6
OPEN = 8
FIRST = 24
LAG = 16
ORDER = (4, 10, 6, 12, 8, 14, 0, 11, 7, 9, 3, 13, 5, 2, 15, 1)


def kernel(n, p, rows, heads, head, kv, q_hbm, k_hbm, v_hbm, out_ref, q_ref, kbuf, vbuf, scores, weights, mine, stat, parts, stats,
           qsem, ksem, vsem, part_send, part_recv, stat_send, stat_recv, out_send, out_recv):
    me = lax.axis_index("sp")
    group = heads // kv
    scale = head ** -0.5

    def other(d):
        return lax.rem(me + d, p)

    def fetch_k(s, slot):
        return pltpu.make_async_copy(k_hbm.at[s], kbuf.at[slot], ksem.at[slot])

    def fetch_v(s, slot):
        return pltpu.make_async_copy(v_hbm.at[s], vbuf.at[slot], vsem.at[slot])

    fetch_q = pltpu.make_async_copy(q_hbm, q_ref, qsem)
    fetch_q.start()
    for s in range(SLOTS):
        fetch_k(s, s).start(priority=1)
        fetch_v(s, s).start(priority=1)

    barrier = pltpu.get_barrier_semaphore()
    for d in range(1, p):
        pl.semaphore_signal(barrier, inc=1, device_id={"sp": other(d)}, device_id_type=MESH)

    row = lax.broadcasted_iota(jnp.int32, (heads, rows), 0)
    col = lax.broadcasted_iota(jnp.int32, (heads, rows), 1)
    own = (col % kv) == (row // group)
    row1 = lax.broadcasted_iota(jnp.int32, (heads, 128), 0)
    col1 = lax.broadcasted_iota(jnp.int32, (heads, 128), 1)
    at_high, at_total = col1 == row1, col1 == row1 + 64

    def owner(s):
        j = lax.rem(s, p)
        return functools.reduce(jnp.add, [jnp.where(j == i, d, 0) for i, d in enumerate(ORDER)])

    def owned(turn):
        return turn * p + functools.reduce(jnp.add, [jnp.where(me == d, i, 0) for i, d in enumerate(ORDER)])

    def score(s, slot):
        scores[...] = lax.dot_general(q_ref[s], kbuf[slot], (((1,), (1,)), ((), ())), preferred_element_type=jnp.float32)

    def soften(s):
        x = jnp.where(own, scores[...], -jnp.inf)
        high = jnp.max(x, axis=1, keepdims=True)
        w = jnp.exp((x - high) * scale)
        weights[...] = w.astype(jnp.bfloat16)
        total = jnp.sum(w, axis=1, keepdims=True)
        spread = jnp.where(at_high, high * scale, jnp.where(at_total, total, 0.0))
        stat[s] = jnp.sum(spread, axis=0, keepdims=True)

    def mix(s, slot, pieces=1):
        step = rows // pieces
        got = [jnp.dot(weights[:, i:i + step], vbuf[slot, i:i + step], preferred_element_type=jnp.float32) for i in range(0, rows, step)]
        mine[s] = functools.reduce(jnp.add, got).astype(jnp.bfloat16)

    def to_owner(s, who, src, dst, send, recv):
        turn = s // p
        place = lax.rem(me - who - 1 + 2 * p, p)

        @pl.when(who != me)
        def _():
            pltpu.make_async_remote_copy(
                src_ref=src.at[s], dst_ref=dst.at[turn, place], send_sem=send, recv_sem=recv.at[turn], device_id={"sp": who}, device_id_type=MESH
            ).start()

    def send_stat(s, who):
        to_owner(s, who, stat, stats, stat_send, stat_recv)

    def send_part(s, who):
        to_owner(s, who, mine, parts, part_send, part_recv)

    def all_of(ref, sem):
        return pltpu.make_async_copy(ref, ref, sem)

    def together(s):
        turn = s // p
        all_of(stats.at[turn], stat_recv.at[turn]).wait()
        rows = [stat[s] if j == p - 1 else stats[turn, j] for j in range(p)]
        top = functools.reduce(jnp.maximum, rows)
        share = [jnp.exp(x - top) for x in rows]
        whole = functools.reduce(jnp.add, [a * pltpu.roll(x, 64, 1) for a, x in zip(share, rows)])
        share = [jnp.sum(jnp.where(at_high, a / whole, 0.0), axis=1, keepdims=True) for a in share]
        all_of(parts.at[turn], part_recv.at[turn]).wait()
        seen = jnp.zeros((heads, head), jnp.float32)
        for j in range(p):
            x = mine[s] if j == p - 1 else parts[turn, j]
            seen = seen + x.astype(jnp.float32) * share[j]
        out_ref[s] = seen.astype(out_ref.dtype)
        for d in sorted(range(1, p), key=lambda d: min(d, p - d)):
            pltpu.make_async_remote_copy(
                src_ref=out_ref.at[s], dst_ref=out_ref.at[s], send_sem=out_send, recv_sem=out_recv, device_id={"sp": other(d)}, device_id_type=MESH
            ).start()

    fetch_q.wait()
    fetch_k(0, 0).wait()
    score(0, 0)
    fetch_k(1, 1).wait()
    soften(0)
    score(1, 1)
    for s in (0, 1):
        fetch_k(s + SLOTS, s).start(priority=1)

    def body(s, before):
        who = owner(s - 1)
        kslot, vslot = lax.rem(s, SLOTS), lax.rem(s - 2, SLOTS)
        fetch_v(s - 2, vslot).wait()
        fetch_k(s, kslot).wait()
        mix(s - 2, vslot)
        soften(s - 1)
        score(s, kslot)

        @pl.when(s + SLOTS < n)
        def _():
            fetch_k(s + SLOTS, kslot).start(priority=1)

        @pl.when(s - 2 + SLOTS < n)
        def _():
            fetch_v(s - 2 + SLOTS, vslot).start(priority=1)

        @pl.when(s == OPEN)
        def _():
            pl.semaphore_wait(barrier, p - 1)

            def late(u, _):
                who = owner(u)
                send_stat(u, who)
                send_part(u, who)
                return 0

            lax.fori_loop(0, OPEN - 2, late, 0)
            send_stat(OPEN - 2, ORDER[(OPEN - 2) % p])

        @pl.when(s >= OPEN)
        def _():
            send_stat(s - 1, who)
            send_part(s - 2, before)

        @pl.when(s == FIRST)
        def _():
            together(owned(0))

        @pl.when((s >= p + LAG) & (owner(jnp.maximum(s - LAG, 0)) == me))
        def _():
            together(s - LAG)

        return who

    lax.fori_loop(2, n, body, jnp.int32(ORDER[0]))
    slot = (n - 2) % SLOTS
    fetch_v(n - 2, slot).wait()
    mix(n - 2, slot, 2)
    soften(n - 1)
    send_stat(n - 1, ORDER[p - 1])
    send_part(n - 2, ORDER[p - 2])
    slot = (n - 1) % SLOTS
    fetch_v(n - 1, slot).wait()
    mix(n - 1, slot, 2)
    send_part(n - 1, ORDER[p - 1])
    @pl.when(owned(1) >= n - LAG)
    def _():
        together(owned(1))

    turns = n // p
    all_of(out_ref.at[pl.ds(0, n - turns)], out_recv).wait()
    all_of(mine.at[pl.ds(0, n - turns)], part_send).wait()
    all_of(stat.at[pl.ds(0, n - turns)], stat_send).wait()
    all_of(out_ref.at[pl.ds(0, turns * (p - 1))], out_send).wait()


def solution(mesh):
    p = mesh.shape["sp"]

    def step(q, k, v):
        n, heads, head = q.shape
        tokens, kv = k.shape[1:3]
        rows = tokens * kv
        turns = n // p
        assert n == 2 * p and sorted(ORDER) == list(range(p)) and FIRST >= p + 2
        return pl.pallas_call(
            functools.partial(kernel, n, p, rows, heads, head, kv),
            out_shape=jax.ShapeDtypeStruct(q.shape, q.dtype),
            in_specs=[pl.BlockSpec(memory_space=pltpu.HBM)] * 3,
            out_specs=pl.BlockSpec(memory_space=pltpu.VMEM),
            scratch_shapes=[
                pltpu.VMEM((n, heads, head), jnp.bfloat16),
                pltpu.VMEM((SLOTS, rows, head), jnp.bfloat16),
                pltpu.VMEM((SLOTS, rows, head), jnp.bfloat16),
                pltpu.VMEM((heads, rows), jnp.float32),
                pltpu.VMEM((heads, rows), jnp.bfloat16),
                pltpu.VMEM((n, heads, head), jnp.bfloat16),
                pltpu.VMEM((n, 1, 128), jnp.float32),
                pltpu.VMEM((turns, p - 1, heads, head), jnp.bfloat16),
                pltpu.VMEM((turns, p - 1, 1, 128), jnp.float32),
                pltpu.SemaphoreType.DMA,
                pltpu.SemaphoreType.DMA((SLOTS,)),
                pltpu.SemaphoreType.DMA((SLOTS,)),
                pltpu.SemaphoreType.DMA,
                pltpu.SemaphoreType.DMA((turns,)),
                pltpu.SemaphoreType.DMA,
                pltpu.SemaphoreType.DMA((turns,)),
                pltpu.SemaphoreType.DMA,
                pltpu.SemaphoreType.DMA,
            ],
            compiler_params=pltpu.CompilerParams(vmem_limit_bytes=48 * 2**20, collective_id=0, has_side_effects=True),
            name="attend",
        )(pltpu.with_memory_space_constraint(q, pltpu.HBM), k.reshape(n, rows, head), v.reshape(n, rows, head))

    return jax.shard_map(
        step,
        mesh=mesh,
        in_specs=(P("dp", None, None), P("dp", "sp", None, None), P("dp", "sp", None, None)),
        out_specs=P("dp", None, None),
        check_vma=False,
    )
```
